32 devices in a mesh: pp: 4 (over y, x), cp: 8 (over z, core).
Axes of the slice: x: 2, y: 2, z: 4, core: 2. Of those that a mesh axis runs over, the one named last changes fastest.
Arguments:
- x_in: bfloat16 [4, 1024, 2048], P(None, 'cp'), may hold values from -60 to 80
- norm_gain: float32 [4, 2048], P('pp'), may hold values from 0.5 to 1.5
- w_qkv: bfloat16 [4, 2048, 3072], P('pp', 'cp'), may hold values from -0.13258252 to 1.307771
- w_out: bfloat16 [4, 2048, 2048], P('pp', 'cp'), may hold values from -0.125 to 0.125
- cycle_size: int32 [4], replicated, may hold values from 2 to 8, as said below
- token_pos: int32 [4, 1024], replicated, may hold values from 0 to 1023, as said below
- doc_starts: int32 [4, 16], replicated, may hold values from 0 to 1024, as said below
Outputs:
- layer_outputs: bfloat16 [4, 4, 1024, 2048], P('pp', None, 'cp')
The draws below stay inside these ranges and needn't reach their ends.
Inputs may be any that keep to these rules, and one draw needn't show every extreme that they name: `cycle_size`: powers of two dividing the devices of cp; some micro-batch has 8 and some has 2. `token_pos`: for a micro-batch with group size r, every aligned block of r * 128 slots holds each position of that block once. `doc_starts`: for a micro-batch with group size r and g below 8 / r, entry 2 g is g * r * 128 and entry 2 g + 1 either lies strictly inside that group's positions or is 1024, so each group holds one or two documents; the remaining entries are 1024.
All inputs are finite; a program needn't handle non-finite values.
Results may differ from the reference program's by a relative error of at most 0.0075.
Values may be sent and summed in bfloat16 or wider, within the bound.
A program may use at most 128 MiB of HBM per device.

```python
import math
import jax
import jax.numpy as jnp
from jax import lax

D = 2048
HEADS = 16
KV_HEADS = 4
HEAD_DIM = 128
T_DEV = 128
MICRO = 4
CYCLE_MAX = 8
LAYERS = 4
TOKENS = 1024
DOCS = 16
QKV_COLS = 3072


def cycle_draw(key):
    levels = CYCLE_MAX.bit_length() - 1
    exponent = jax.random.randint(key, (MICRO,), 1, levels + 1).astype(jnp.int32)
    sizes_drawn = jnp.left_shift(jnp.int32(1), exponent)
    chosen = jax.random.randint(jax.random.fold_in(key, 1), (), 0, MICRO)
    other = (chosen + jax.random.randint(jax.random.fold_in(key, 2), (), 1, MICRO)) % MICRO
    index = jnp.arange(MICRO)
    sizes_drawn = jnp.where(index == other, 2, sizes_drawn)
    return jnp.where(index == chosen, CYCLE_MAX, sizes_drawn).astype(jnp.int32)


def draw_cycle_size(key, part):
    return cycle_draw(jax.random.fold_in(key, 11))


def draw_token_pos(key, part):
    cycles = cycle_draw(jax.random.fold_in(key, 11))

    def one_row(row_key, cycle_devices):
        span = cycle_devices * T_DEV
        slots = jnp.arange(TOKENS, dtype=jnp.int32)
        groups = slots // span
        noise = jax.random.permutation(row_key, TOKENS).astype(jnp.int32)
        ordered = jnp.argsort(groups * TOKENS + noise, stable=True)
        return jnp.zeros((TOKENS,), jnp.int32).at[ordered].set(slots)
    row_keys = jax.random.split(jax.random.fold_in(key, 12), MICRO)
    return jax.vmap(one_row)(row_keys, cycles)


def draw_doc_starts(key, part):
    cycles = cycle_draw(jax.random.fold_in(key, 11))
    group_slots = DOCS // 2

    def one_row(row_key, cycle_devices):
        span = cycle_devices * T_DEV
        live_groups = group_slots // cycle_devices
        index = jnp.arange(group_slots, dtype=jnp.int32)
        inside = jax.random.randint(row_key, (group_slots,), 1, span).astype(jnp.int32)
        split_here = jax.random.randint(jax.random.fold_in(row_key, 5), (group_slots,), 0, 2) == 1
        first_pos = index * span
        second_pos = jnp.where(split_here, first_pos + inside, TOKENS)
        paired = jnp.stack([first_pos, second_pos], axis=1).reshape(-1)
        live = jnp.repeat(index < live_groups, 2)
        return jnp.where(live, paired, TOKENS).astype(jnp.int32)
    row_keys = jax.random.split(jax.random.fold_in(key, 13), MICRO)
    return jax.vmap(one_row)(row_keys, cycles)


def draw_x_in(key, part):
    base_draw = jnp.clip(jax.random.normal(jax.random.fold_in(key, 21), (MICRO, TOKENS, D), jnp.float32), -6.0, 6.0)
    return base_draw.astype(jnp.bfloat16)


def draw_w_qkv(key, part):
    base_draw = jnp.clip(jax.random.normal(jax.random.fold_in(key, 31), (LAYERS, D, QKV_COLS), jnp.float32), -6.0, 6.0) * D ** (-0.5)
    return base_draw.astype(jnp.bfloat16)


def block_levels(rng, extent, shards, smallest, top_value):
    def one(position, blocks):
        draws = jax.random.uniform(jax.random.fold_in(jax.random.fold_in(rng, 6), position), (blocks,), jnp.float32, smallest / len(shards), top_value / len(shards))
        return jnp.repeat(jnp.exp(draws), extent[position] // blocks).reshape((-1,) + (1,) * (len(extent) - position - 1))

    gain = one(*shards[0])
    for cut in shards[1:]:
        gain = gain * one(*cut)
    return gain


def centred(stream_key, extent, width, bound, cuts=(), held_as=jnp.bfloat16):
    gain = block_levels(stream_key, extent, cuts, -0.22, 0.18) if cuts else 1.0
    array = jax.random.normal(stream_key, extent, jnp.float32) * width * gain
    return jnp.minimum(jnp.maximum(array, -bound), bound).astype(held_as)


def setup_inputs(seed: int = 0) -> dict:
    seeds = jax.random.split(jax.random.key(seed), 8)
    return {
        "x_in": draw_x_in(jax.random.fold_in(seeds[7], 71), 0),
        "norm_gain": jnp.clip(1.0 + 0.1 * jax.random.normal(seeds[1], (LAYERS, D), jnp.float32), 0.5, 1.5),
        "w_qkv": draw_w_qkv(jax.random.fold_in(seeds[7], 71), 0),
        "w_out": centred(seeds[3], (LAYERS, HEADS * HEAD_DIM, D), (HEADS * HEAD_DIM) ** -0.5, 0.125, ((0, 4), (1, 8))),
        "cycle_size": draw_cycle_size(jax.random.fold_in(seeds[7], 71), 0),
        "token_pos": draw_token_pos(jax.random.fold_in(seeds[7], 71), 0),
        "doc_starts": draw_doc_starts(jax.random.fold_in(seeds[7], 71), 0),
    }


epsilon = 1e-05
rope_base = 500000.0

def rotate(values, relative):
    half_dim = values.shape[-1] // 2
    frequency_index = jnp.arange(half_dim, dtype=jnp.float32)
    inverse = jnp.power(jnp.float32(rope_base), -2.0 * frequency_index / values.shape[-1])
    angles = relative.astype(jnp.float32)[:, None] * inverse[None, :]
    cosine = jnp.cos(angles)[:, None, :]
    sine_part = jnp.sin(angles)[:, None, :]
    first_half = values[..., :half_dim]
    second_half = values[..., half_dim:]
    return jnp.concatenate([first_half * cosine - second_half * sine_part, second_half * cosine + first_half * sine_part], axis=-1)

def doc_begin(positions, starts):
    at_or_below = starts[None, :] <= positions[:, None]
    return lax.optimization_barrier(jnp.max(jnp.where(at_or_below, starts[None, :], 0), axis=1)).astype(jnp.int32)

def layer_forward(hidden, gain_row, qkv_weight, out_weight, positions, starts, cycle_devices):
    widened = hidden.astype(jnp.float32)
    mean_square = lax.optimization_barrier(jnp.mean(widened * widened, axis=-1, keepdims=True))
    normed = (widened * lax.rsqrt(mean_square + epsilon) * gain_row.astype(jnp.float32)).astype(jnp.bfloat16)
    projected = jnp.dot(normed, qkv_weight, preferred_element_type=jnp.float32)
    query_cols = HEADS * HEAD_DIM
    key_cols = KV_HEADS * HEAD_DIM
    begins = doc_begin(positions, starts)
    relative = positions - begins
    queries = rotate(projected[:, :query_cols].reshape(-1, HEADS, HEAD_DIM), relative).astype(jnp.bfloat16)
    keys_all = rotate(projected[:, query_cols:query_cols + key_cols].reshape(-1, KV_HEADS, HEAD_DIM), relative).astype(jnp.bfloat16)
    values_all = projected[:, query_cols + key_cols:].reshape(-1, KV_HEADS, HEAD_DIM).astype(jnp.bfloat16)
    groups = positions // (cycle_devices * T_DEV)
    window = CYCLE_MAX * T_DEV
    block_rows = math.gcd(window, 512)
    block_count = TOKENS // block_rows

    def attend(pieces):
        block_queries, block_pos, block_begin, block_group, block_number = pieces
        window_start = (block_number * block_rows // window * window).astype(jnp.int32)
        near_keys = lax.dynamic_slice_in_dim(keys_all, window_start, window, 0)
        near_values = lax.dynamic_slice_in_dim(values_all, window_start, window, 0)
        near_pos = lax.dynamic_slice_in_dim(positions, window_start, window, 0)
        near_begin = lax.dynamic_slice_in_dim(begins, window_start, window, 0)
        near_group = lax.dynamic_slice_in_dim(groups, window_start, window, 0)
        grouped = block_queries.astype(jnp.float32).reshape(block_rows, KV_HEADS, HEADS // KV_HEADS, HEAD_DIM)
        scores = jnp.einsum('bkgd,skd->kgbs', grouped, near_keys.astype(jnp.float32)) * HEAD_DIM ** (-0.5)
        visible = (block_group[:, None] == near_group[None, :]) & (block_begin[:, None] == near_begin[None, :]) & (near_pos[None, :] <= block_pos[:, None])
        scores = jnp.where(visible[None, None], scores, -1e+30)
        row_max = lax.optimization_barrier(jnp.max(scores, axis=-1, keepdims=True))
        weights_exp = jnp.exp(scores - row_max)
        row_sum = lax.optimization_barrier(jnp.sum(weights_exp, axis=-1, keepdims=True))
        rounded = lax.optimization_barrier(weights_exp.astype(jnp.bfloat16)).astype(jnp.float32)
        combined = jnp.einsum('kgbs,skd->kgbd', rounded, near_values.astype(jnp.float32)) / row_sum
        return jnp.transpose(combined, (2, 0, 1, 3)).reshape(block_rows, query_cols).astype(jnp.bfloat16)
    attended = lax.map(attend, (queries.reshape(block_count, block_rows, HEADS, HEAD_DIM), positions.reshape(block_count, block_rows), begins.reshape(block_count, block_rows), groups.reshape(block_count, block_rows), jnp.arange(block_count, dtype=jnp.int32)))
    attended = attended.reshape(TOKENS, query_cols)
    output = jnp.dot(attended, out_weight, preferred_element_type=jnp.float32)
    return (widened + output).astype(jnp.bfloat16)

def reference(x_in, norm_gain, w_qkv, w_out, cycle_size, token_pos, doc_starts):
    per_micro = []
    for micro_index in range(MICRO):
        hidden = x_in[micro_index]
        layer_rows = []
        for layer_index in range(LAYERS):
            hidden = layer_forward(hidden, norm_gain[layer_index], w_qkv[layer_index], w_out[layer_index], token_pos[micro_index], doc_starts[micro_index], cycle_size[micro_index])
            layer_rows.append(hidden)
        per_micro.append(jnp.stack(layer_rows))
    return jnp.stack(per_micro, axis=1)
```

```python
import functools
import math

import jax
import jax.numpy as jnp
from jax import lax
from jax.experimental import pallas as pl
from jax.experimental.pallas import tpu as pltpu
from jax.sharding import PartitionSpec as P

HEADS = 16
KV_HEADS = 4
HEAD_DIM = 128
CYCLE_MAX = 8
CORES = 2
TILE = 256

epsilon = 1e-05
rope_base = 500000.0
MESH = pl.DeviceIdType.MESH


def kernel(
    chips, sections, x_ref, gain_ref, wq_in, wo_in, cos_ref, sin_ref, pos_q, code_q, pos_k, code_k,
    out_ref,
    wq, wo, hid, nrm, qs, kv, att, res, bias,
    w_swap_s, w_swap_r, w_right_s, w_right_r, w_left_s, w_left_r,
    x_s, x_r, loc, hop_s, hop_r, relay_s, relay_r, kv_s, kv_r, att_s, att_r, o_s, o_r,
):
    micro, tok, width = x_ref.shape
    rows = wq_in.shape[1]
    half = width // 2
    q_cols = HEADS // CORES * HEAD_DIM
    kv_cols = KV_HEADS // CORES * HEAD_DIM
    heads = HEADS // CORES
    per_kv = HEADS // KV_HEADS
    peers = CYCLE_MAX // CORES
    tiles = half // TILE
    section = lax.axis_index("pp")
    cp = lax.axis_index("cp")
    chip = cp // CORES
    core = cp % CORES
    partner = {"cp": chip * CORES + 1 - core}
    place = chip % peers
    base = chip - place
    first = section == 0
    last = section == sections - 1

    def remote(src, dst, s, r, device):
        return pltpu.make_async_remote_copy(
            src_ref=src, dst_ref=dst, send_sem=s, recv_sem=r, device_id=device, device_id_type=MESH
        )

    def block(w, index, count):
        return w.at[pl.ds(pl.multiple_of(index * rows, rows), count * rows), :]

    weights = ((wq_in, wq), (wo_in, wo))

    def swap(a):
        src, w = weights[a]
        return remote(src.at[1 - core], block(w, cp, 1), w_swap_s.at[a], w_swap_r.at[a], partner)

    def swap_in(a):
        src, w = weights[a]
        there = chip * CORES + 1 - core
        return remote(src.at[core], block(w, there, 1), w_swap_s.at[a], w_swap_r.at[a], partner)

    def right(a, index):
        piece = block(weights[a][1], index * CORES, CORES)
        return remote(piece, piece, w_right_s.at[a, index], w_right_r.at[a, index],
                      {"cp": (chip + 1) * CORES + core})

    def left(a, index):
        piece = block(weights[a][1], index * CORES, CORES)
        return remote(piece, piece, w_left_s.at[a, index], w_left_r.at[a, index],
                      {"cp": (chip - 1) * CORES + core})

    def own(a):
        src, w = weights[a]
        return pltpu.make_async_copy(src.at[core], block(w, cp, 1), loc.at[a])

    def send_own(a):
        @pl.when(chip < chips - 1)
        def _():
            right(a, chip).start()

        @pl.when(chip > 0)
        def _():
            left(a, chip).start()

    def relay_weights(a):
        def step(i, carry):
            @pl.when(i <= chip)
            def _():
                right(a, chip - i).wait_recv()

                @pl.when(chip < chips - 1)
                def _():
                    right(a, chip - i).start()

            @pl.when(chip + i <= chips - 1)
            def _():
                left(a, chip + i).wait_recv()

                @pl.when(chip > 0)
                def _():
                    left(a, chip + i).start()

            return carry

        lax.fori_loop(1, chips, step, 0)

    def finish_weights(a):
        swap(a).wait_send()

        def step(i, carry):
            @pl.when((i <= chip) & (chip < chips - 1))
            def _():
                right(a, i).wait_send()

            @pl.when((i >= chip) & (chip > 0))
            def _():
                left(a, i).wait_send()

            return carry

        lax.fori_loop(0, chips, step, 0)

    own_rows = pl.ds(pl.multiple_of(core * tok, tok), tok)
    other_rows = pl.ds(pl.multiple_of((1 - core) * tok, tok), tok)

    def x_local(m, h):
        return pltpu.make_async_copy(
            x_ref.at[m, :, pl.ds(h * half, half)], hid.at[m, h, own_rows, :], loc.at[2 + m * 2 + h])

    def x_send(m, h):
        return remote(x_ref.at[m, :, pl.ds(h * half, half)], hid.at[m, h, own_rows, :],
                      x_s.at[m, h], x_r.at[m, h], partner)

    def x_wait(m, h):
        piece = hid.at[m, h, other_rows, :]
        return remote(piece, piece, x_s.at[m, h], x_r.at[m, h], partner)

    def cols(t):
        return pl.ds(pl.multiple_of(t * TILE, TILE), TILE)

    def hop(m, t):
        return remote(res.at[m, :, cols(t)], hid.at[m, core, :, cols(t)],
                      hop_s.at[m, t], hop_r.at[m, t], {"pp": section + 1})

    def relay(m, t):
        return remote(hid.at[m, core, :, cols(t)], hid.at[m, core, :, cols(t)],
                      relay_s.at[m, t], relay_r.at[m, t], partner)

    def relay_in(m, t):
        piece = hid.at[m, 1 - core, :, cols(t)]
        return remote(piece, piece, relay_s.at[m, t], relay_r.at[m, t], partner)

    def kv_send(m, d):
        there = lax.rem(place + d, peers)
        return remote(kv.at[m, place], kv.at[m, place], kv_s.at[m, d - 1], kv_r.at[m, d - 1],
                      {"cp": (base + there) * CORES + core})

    def kv_in(m, d):
        source = lax.rem(place - d + peers, peers)
        return remote(kv.at[m, source], kv.at[m, source], kv_s.at[m, d - 1], kv_r.at[m, d - 1],
                      {"cp": (base + source) * CORES + core})

    def att_send(m, g):
        c = pl.ds(g * per_kv * HEAD_DIM, per_kv * HEAD_DIM)
        return remote(att.at[m, core, :, c], att.at[m, core, :, c], att_s.at[m, g], att_r.at[m, g], partner)

    def att_in(m, g):
        c = pl.ds(g * per_kv * HEAD_DIM, per_kv * HEAD_DIM)
        piece = att.at[m, 1 - core, :, c]
        return remote(piece, piece, att_s.at[m, g], att_r.at[m, g], partner)

    def out_send(m):
        return remote(res.at[m, other_rows, :], out_ref.at[m, :, pl.ds(pl.multiple_of(core * half, half), half)],
                      o_s.at[m], o_r.at[m], partner)

    def out_in(m):
        return remote(res.at[m, own_rows, :],
                      out_ref.at[m, :, pl.ds(pl.multiple_of((1 - core) * half, half), half)],
                      o_s.at[m], o_r.at[m], partner)

    swap(0).start()
    swap(1).start()
    own(0).start()
    own(1).start()
    own(0).wait()
    swap_in(0).wait_recv()
    send_own(0)

    @pl.when(first)
    def _():
        for m in range(micro):
            for h in range(2):
                x_send(m, h).start()
                x_local(m, h).start()

    own(1).wait()
    swap_in(1).wait_recv()
    relay_weights(0)
    send_own(1)

    def rope(values, m):
        return values * cos_ref[m] + pltpu.roll(values, HEAD_DIM // 2, 1) * sin_ref[m]

    def front(m):
        @pl.when(first)
        def _():
            for h in range(2):
                x_local(m, h).wait()
                x_wait(m, h).wait_recv()

        @pl.when(section > 0)
        def _():
            for t in range(tiles):
                hop(m, t).wait_recv()
                relay(m, t).start()
            for t in range(tiles):
                relay_in(m, t).wait_recv()

        low = hid[m, 0].astype(jnp.float32)
        high = hid[m, 1].astype(jnp.float32)
        total = jnp.sum(low * low, axis=1, keepdims=True) + jnp.sum(high * high, axis=1, keepdims=True)
        scale = lax.rsqrt(total / width + epsilon)
        nrm[:, :half] = (low * scale * gain_ref[:, :half]).astype(jnp.bfloat16)
        nrm[:, half:] = (high * scale * gain_ref[:, half:]).astype(jnp.bfloat16)
        keys = jnp.dot(nrm[...], wq[:, q_cols : q_cols + kv_cols], preferred_element_type=jnp.float32)
        for g in range(KV_HEADS // CORES):
            c = slice(g * HEAD_DIM, (g + 1) * HEAD_DIM)
            kv[m, place, :, c] = rope(keys[:, c], m).astype(jnp.bfloat16)
        values = jnp.dot(nrm[...], wq[:, q_cols + kv_cols :], preferred_element_type=jnp.float32)
        kv[m, place, :, kv_cols:] = values.astype(jnp.bfloat16)
        for d in range(1, peers):
            kv_send(m, d).start()

        def q_tile(t, carry):
            part = jnp.dot(nrm[...], wq[:, cols(t)], preferred_element_type=jnp.float32)
            for g in range(TILE // HEAD_DIM):
                c = slice(g * HEAD_DIM, (g + 1) * HEAD_DIM)
                qs[m, t * (TILE // HEAD_DIM) + g] = rope(part[:, c], m).astype(jnp.bfloat16)
            return carry

        lax.fori_loop(0, q_cols // TILE, q_tile, 0)

    factor = HEAD_DIM ** (-0.5) * math.log2(math.e)

    def back(m):
        visible = (code_q[m] == code_k[m]) & (pos_k[m] <= pos_q[m])
        bias[...] = jnp.where(visible, 0.0, -1e30).astype(jnp.float32)
        for d in range(1, peers):
            kv_in(m, d).wait_recv()
        for g in range(KV_HEADS // CORES):
            c = slice(g * HEAD_DIM, (g + 1) * HEAD_DIM)
            v = slice(kv_cols + g * HEAD_DIM, kv_cols + (g + 1) * HEAD_DIM)
            for j in range(per_kv):
                h = g * per_kv + j
                key_block = kv[m, :, :, c].reshape(peers * CORES * tok, HEAD_DIM)
                value_block = kv[m, :, :, v].reshape(peers * CORES * tok, HEAD_DIM)
                scores = lax.dot_general(
                    qs[m, h], key_block, (((1,), (1,)), ((), ())), preferred_element_type=jnp.float32
                ) + bias[...]
                top = jnp.max(scores, axis=1, keepdims=True)
                weights_exp = jnp.exp2((scores - top) * factor)
                row_sum = jnp.sum(weights_exp, axis=1, keepdims=True)
                combined = jnp.dot(
                    weights_exp.astype(jnp.bfloat16), value_block, preferred_element_type=jnp.float32
                )
                att[m, core, :, h * HEAD_DIM : (h + 1) * HEAD_DIM] = (combined / row_sum).astype(jnp.bfloat16)
            att_send(m, g).start()

        @pl.when(m == 0)
        def _():
            relay_weights(1)

        for g in range(KV_HEADS // CORES):
            att_in(m, g).wait_recv()

        def out_tile(t, carry):
            total = jnp.dot(att[m, 0], wo[:half, cols(t)], preferred_element_type=jnp.float32)
            total += jnp.dot(att[m, 1], wo[half:, cols(t)], preferred_element_type=jnp.float32)
            result = (hid[m, core, :, cols(t)].astype(jnp.float32) + total).astype(jnp.bfloat16)
            res[m, :, cols(t)] = result

            @pl.when(section < sections - 1)
            def _():
                hop(m, t).start()

            place_cols = pl.ds(pl.multiple_of(core * half + t * TILE, TILE), TILE)
            out_ref[m, :, place_cols] = res[m, own_rows, cols(t)]
            return carry

        lax.fori_loop(0, tiles, out_tile, 0)
        out_send(m).start()

    def turn(i, carry):
        @pl.when(i < micro)
        def _():
            front(i)

        @pl.when(i > 0)
        def _():
            back(i - 1)

        return carry

    lax.fori_loop(0, micro + 1, turn, 0)

    finish_weights(0)
    finish_weights(1)

    def finish(m, carry):
        @pl.when(first)
        def _():
            for h in range(2):
                x_send(m, h).wait_send()

        @pl.when(section > 0)
        def _():
            for t in range(tiles):
                relay(m, t).wait_send()

        @pl.when(section < sections - 1)
        def _():
            for t in range(tiles):
                hop(m, t).wait_send()

        for d in range(1, peers):
            kv_send(m, d).wait_send()
        for g in range(KV_HEADS // CORES):
            att_send(m, g).wait_send()
        out_send(m).wait_send()
        out_in(m).wait_recv()
        return carry

    lax.fori_loop(0, micro, finish, 0)


def doc_begin(positions, starts):
    at_or_below = starts[:, None, :] <= positions[:, :, None]
    return jnp.max(jnp.where(at_or_below, starts[:, None, :], 0), axis=2)


def body(x_in, norm_gain, w_qkv, w_out, cycle_size, token_pos, doc_starts):
    sections = lax.axis_size("pp")
    chips = lax.axis_size("cp") // CORES
    device = lax.axis_index("cp")
    micro, tok, width = x_in.shape
    rows = w_qkv.shape[1]
    total_tokens = token_pos.shape[1]
    half = width // 2
    query_cols = HEADS * HEAD_DIM
    key_cols = KV_HEADS * HEAD_DIM
    window = CYCLE_MAX * tok
    pair = CORES * tok

    block_start = device // CYCLE_MAX * window
    key_pos = lax.dynamic_slice_in_dim(token_pos, block_start, window, 1)
    key_begin = doc_begin(key_pos, doc_starts)
    key_code = key_pos // (cycle_size * tok)[:, None] * (total_tokens + 1) + key_begin
    inside = device % CYCLE_MAX // CORES * pair
    query_pos = lax.dynamic_slice_in_dim(key_pos, inside, pair, 1)
    query_begin = lax.dynamic_slice_in_dim(key_begin, inside, pair, 1)
    query_code = lax.dynamic_slice_in_dim(key_code, inside, pair, 1)
    frequency_index = jnp.arange(HEAD_DIM // 2, dtype=jnp.float32)
    inverse = jnp.power(jnp.float32(rope_base), -2.0 * frequency_index / HEAD_DIM)
    angles = (query_pos - query_begin).astype(jnp.float32)[:, :, None] * inverse
    cosine, sine = jnp.cos(angles), jnp.sin(angles)
    cos_full = jnp.concatenate([cosine, cosine], axis=-1)
    sin_full = jnp.concatenate([-sine, sine], axis=-1)

    def split(array):
        return jnp.stack(jnp.split(array, CORES, axis=1))

    wq_split = jnp.concatenate(
        [
            split(w_qkv[0][:, :query_cols]),
            split(w_qkv[0][:, query_cols : query_cols + key_cols]),
            split(w_qkv[0][:, query_cols + key_cols :]),
        ],
        axis=2,
    )
    wo_split = split(w_out[0])

    peers = CYCLE_MAX // CORES
    tiles = half // TILE
    bf = jnp.bfloat16
    dma = pltpu.SemaphoreType.DMA
    vmem = pl.BlockSpec(memory_space=pltpu.VMEM)
    outputs = pl.pallas_call(
        functools.partial(kernel, chips, sections),
        out_shape=jax.ShapeDtypeStruct((micro, tok, width), bf),
        in_specs=[vmem] * 10,
        out_specs=vmem,
        scratch_shapes=[
            pltpu.VMEM((width, wq_split.shape[2]), bf),
            pltpu.VMEM((query_cols, half), bf),
            pltpu.VMEM((micro, 2, pair, half), bf),
            pltpu.VMEM((pair, width), bf),
            pltpu.VMEM((micro, HEADS // CORES, pair, HEAD_DIM), bf),
            pltpu.VMEM((micro, peers, pair, 2 * key_cols // CORES), bf),
            pltpu.VMEM((micro, CORES, pair, query_cols // CORES), bf),
            pltpu.VMEM((micro, pair, half), bf),
            pltpu.VMEM((pair, window), jnp.float32),
            dma((2,)), dma((2,)),
            dma((2, chips)), dma((2, chips)), dma((2, chips)), dma((2, chips)),
            dma((micro, 2)), dma((micro, 2)),
            dma((2 + 2 * micro,)),
            dma((micro, tiles)), dma((micro, tiles)),
            dma((micro, tiles)), dma((micro, tiles)),
            dma((micro, peers - 1)), dma((micro, peers - 1)),
            dma((micro, KV_HEADS // CORES)), dma((micro, KV_HEADS // CORES)),
            dma((micro,)), dma((micro,)),
        ],
        compiler_params=pltpu.CompilerParams(has_side_effects=True, vmem_limit_bytes=60 * 1024 * 1024),
    )(
        x_in, norm_gain, wq_split, wo_split, cos_full, sin_full,
        query_pos[:, :, None], query_code[:, :, None], key_pos[:, None, :], key_code[:, None, :],
    )
    return outputs[None]


def solution(mesh):
    in_specs = (
        P(None, "cp", None),
        P("pp", None),
        P("pp", "cp", None),
        P("pp", "cp", None),
        P(),
        P(),
        P(),
    )
    out_specs = P("pp", None, "cp", None)
    return jax.shard_map(body, mesh=mesh, in_specs=in_specs, out_specs=out_specs, check_vma=False)
```

```python
import functools
import math

import jax
import jax.numpy as jnp
from jax import lax
from jax.experimental import pallas as pl
from jax.experimental.pallas import tpu as pltpu
from jax.sharding import PartitionSpec as P

HEADS = 16
KV_HEADS = 4
HEAD_DIM = 128
CYCLE_MAX = 8
CORES = 2
TILE = 256

epsilon = 1e-05
rope_base = 500000.0
MESH = pl.DeviceIdType.MESH


def kernel(
    chips, sections, x_ref, gain_ref, wq_in, wo_in, cos_ref, sin_ref, pos_q, code_q, pos_k, code_k,
    out_ref,
    wq, wo, hid, nrm, qs, kv, att, res, bias,
    w_swap_s, w_swap_r, w_right_s, w_right_r, w_left_s, w_left_r,
    x_s, x_r, loc, hop_s, hop_r, relay_s, relay_r, kv_s, kv_r, att_s, att_r, o_s, o_r,
):
    micro, tok, width = x_ref.shape
    rows = wq_in.shape[1]
    half = width // 2
    q_cols = HEADS // CORES * HEAD_DIM
    kv_cols = KV_HEADS // CORES * HEAD_DIM
    heads = HEADS // CORES
    per_kv = HEADS // KV_HEADS
    peers = CYCLE_MAX // CORES
    tiles = half // TILE
    section = lax.axis_index("pp")
    cp = lax.axis_index("cp")
    chip = cp // CORES
    core = cp % CORES
    partner = {"cp": chip * CORES + 1 - core}
    place = chip % peers
    base = chip - place
    first = section == 0
    last = section == sections - 1

    def remote(src, dst, s, r, device):
        return pltpu.make_async_remote_copy(
            src_ref=src, dst_ref=dst, send_sem=s, recv_sem=r, device_id=device, device_id_type=MESH
        )

    def block(w, index, count):
        return w.at[pl.ds(pl.multiple_of(index * rows, rows), count * rows), :]

    weights = ((wq_in, wq), (wo_in, wo))

    def swap(a):
        src, w = weights[a]
        return remote(src.at[1 - core], block(w, cp, 1), w_swap_s.at[a], w_swap_r.at[a], partner)

    def swap_in(a):
        src, w = weights[a]
        there = chip * CORES + 1 - core
        return remote(src.at[core], block(w, there, 1), w_swap_s.at[a], w_swap_r.at[a], partner)

    def right(a, index):
        piece = block(weights[a][1], index * CORES, CORES)
        return remote(piece, piece, w_right_s.at[a, index], w_right_r.at[a, index],
                      {"cp": (chip + 1) * CORES + core})

    def left(a, index):
        piece = block(weights[a][1], index * CORES, CORES)
        return remote(piece, piece, w_left_s.at[a, index], w_left_r.at[a, index],
                      {"cp": (chip - 1) * CORES + core})

    def own(a):
        src, w = weights[a]
        return pltpu.make_async_copy(src.at[core], block(w, cp, 1), loc.at[a])

    def send_own(a):
        @pl.when(chip < chips - 1)
        def _():
            right(a, chip).start()

        @pl.when(chip > 0)
        def _():
            left(a, chip).start()

    def relay_weights(a):
        def step(i, carry):
            @pl.when(i <= chip)
            def _():
                right(a, chip - i).wait_recv()

                @pl.when(chip < chips - 1)
                def _():
                    right(a, chip - i).start()

            @pl.when(chip + i <= chips - 1)
            def _():
                left(a, chip + i).wait_recv()

                @pl.when(chip > 0)
                def _():
                    left(a, chip + i).start()

            return carry

        lax.fori_loop(1, chips, step, 0)

    def finish_weights(a):
        swap(a).wait_send()

        def step(i, carry):
            @pl.when((i <= chip) & (chip < chips - 1))
            def _():
                right(a, i).wait_send()

            @pl.when((i >= chip) & (chip > 0))
            def _():
                left(a, i).wait_send()

            return carry

        lax.fori_loop(0, chips, step, 0)

    own_rows = pl.ds(pl.multiple_of(core * tok, tok), tok)
    other_rows = pl.ds(pl.multiple_of((1 - core) * tok, tok), tok)

    def x_local(m, h):
        return pltpu.make_async_copy(
            x_ref.at[m, :, pl.ds(h * half, half)], hid.at[m, h, own_rows, :], loc.at[2 + m * 2 + h])

    def x_send(m, h):
        return remote(x_ref.at[m, :, pl.ds(h * half, half)], hid.at[m, h, own_rows, :],
                      x_s.at[m, h], x_r.at[m, h], partner)

    def x_wait(m, h):
        piece = hid.at[m, h, other_rows, :]
        return remote(piece, piece, x_s.at[m, h], x_r.at[m, h], partner)

    def cols(t):
        return pl.ds(pl.multiple_of(t * TILE, TILE), TILE)

    def hop(m, t):
        return remote(res.at[m, :, cols(t)], hid.at[m, core, :, cols(t)],
                      hop_s.at[m, t], hop_r.at[m, t], {"pp": section + 1})

    def relay(m, t):
        return remote(hid.at[m, core, :, cols(t)], hid.at[m, core, :, cols(t)],
                      relay_s.at[m, t], relay_r.at[m, t], partner)

    def relay_in(m, t):
        piece = hid.at[m, 1 - core, :, cols(t)]
        return remote(piece, piece, relay_s.at[m, t], relay_r.at[m, t], partner)

    def kv_send(m, d):
        there = lax.rem(place + d, peers)
        return remote(kv.at[m, place], kv.at[m, place], kv_s.at[m, d - 1], kv_r.at[m, d - 1],
                      {"cp": (base + there) * CORES + core})

    def kv_in(m, d):
        source = lax.rem(place - d + peers, peers)
        return remote(kv.at[m, source], kv.at[m, source], kv_s.at[m, d - 1], kv_r.at[m, d - 1],
                      {"cp": (base + source) * CORES + core})

    def att_send(m, g):
        c = pl.ds(g * per_kv * HEAD_DIM, per_kv * HEAD_DIM)
        return remote(att.at[m, core, :, c], att.at[m, core, :, c], att_s.at[m, g], att_r.at[m, g], partner)

    def att_in(m, g):
        c = pl.ds(g * per_kv * HEAD_DIM, per_kv * HEAD_DIM)
        piece = att.at[m, 1 - core, :, c]
        return remote(piece, piece, att_s.at[m, g], att_r.at[m, g], partner)

    def out_send(m):
        return remote(res.at[m, other_rows, :], out_ref.at[m, :, pl.ds(pl.multiple_of(core * half, half), half)],
                      o_s.at[m], o_r.at[m], partner)

    def out_in(m):
        return remote(res.at[m, own_rows, :],
                      out_ref.at[m, :, pl.ds(pl.multiple_of((1 - core) * half, half), half)],
                      o_s.at[m], o_r.at[m], partner)

    swap(0).start()
    swap(1).start()
    own(0).start()
    own(1).start()
    own(0).wait()
    swap_in(0).wait_recv()
    send_own(0)

    @pl.when(first)
    def _():
        for m in range(micro):
            for h in range(2):
                x_send(m, h).start()
                x_local(m, h).start()

    own(1).wait()
    swap_in(1).wait_recv()
    relay_weights(0)
    send_own(1)

    @pl.when(section > 0)
    def _():
        relay_weights(1)

    def rope(values, m):
        return values * cos_ref[m] + pltpu.roll(values, HEAD_DIM // 2, 1) * sin_ref[m]

    def front(m):
        @pl.when(first)
        def _():
            for h in range(2):
                x_local(m, h).wait()
                x_wait(m, h).wait_recv()

        @pl.when(section > 0)
        def _():
            for t in range(tiles):
                hop(m, t).wait_recv()
                relay(m, t).start()
            for t in range(tiles):
                relay_in(m, t).wait_recv()

        low = hid[m, 0].astype(jnp.float32)
        high = hid[m, 1].astype(jnp.float32)
        total = jnp.sum(low * low, axis=1, keepdims=True) + jnp.sum(high * high, axis=1, keepdims=True)
        scale = lax.rsqrt(total / width + epsilon)
        nrm[:, :half] = (low * scale * gain_ref[:, :half]).astype(jnp.bfloat16)
        nrm[:, half:] = (high * scale * gain_ref[:, half:]).astype(jnp.bfloat16)
        keys = jnp.dot(nrm[...], wq[:, q_cols : q_cols + kv_cols], preferred_element_type=jnp.float32)
        for g in range(KV_HEADS // CORES):
            c = slice(g * HEAD_DIM, (g + 1) * HEAD_DIM)
            kv[m, place, :, c] = rope(keys[:, c], m).astype(jnp.bfloat16)
        values = jnp.dot(nrm[...], wq[:, q_cols + kv_cols :], preferred_element_type=jnp.float32)
        kv[m, place, :, kv_cols:] = values.astype(jnp.bfloat16)
        for d in range(1, peers):
            kv_send(m, d).start()

        def q_tile(t, carry):
            part = jnp.dot(nrm[...], wq[:, cols(t)], preferred_element_type=jnp.float32)
            for g in range(TILE // HEAD_DIM):
                c = slice(g * HEAD_DIM, (g + 1) * HEAD_DIM)
                qs[m, t * (TILE // HEAD_DIM) + g] = rope(part[:, c], m).astype(jnp.bfloat16)
            return carry

        lax.fori_loop(0, q_cols // TILE, q_tile, 0)

    factor = HEAD_DIM ** (-0.5) * math.log2(math.e)

    def back(m):
        visible = (code_q[m] == code_k[m]) & (pos_k[m] <= pos_q[m])
        bias[...] = jnp.where(visible, 0.0, -1e30).astype(jnp.float32)
        for d in range(1, peers):
            kv_in(m, d).wait_recv()
        for g in range(KV_HEADS // CORES):
            c = slice(g * HEAD_DIM, (g + 1) * HEAD_DIM)
            v = slice(kv_cols + g * HEAD_DIM, kv_cols + (g + 1) * HEAD_DIM)
            for j in range(per_kv):
                h = g * per_kv + j
                key_block = kv[m, :, :, c].reshape(peers * CORES * tok, HEAD_DIM)
                value_block = kv[m, :, :, v].reshape(peers * CORES * tok, HEAD_DIM)
                scores = lax.dot_general(
                    qs[m, h], key_block, (((1,), (1,)), ((), ())), preferred_element_type=jnp.float32
                ) + bias[...]
                top = jnp.max(scores, axis=1, keepdims=True)
                weights_exp = jnp.exp2((scores - top) * factor)
                row_sum = jnp.sum(weights_exp, axis=1, keepdims=True)
                combined = jnp.dot(
                    weights_exp.astype(jnp.bfloat16), value_block, preferred_element_type=jnp.float32
                )
                att[m, core, :, h * HEAD_DIM : (h + 1) * HEAD_DIM] = (combined / row_sum).astype(jnp.bfloat16)
            att_send(m, g).start()

        @pl.when(first & (m == 0))
        def _():
            relay_weights(1)

        for g in range(KV_HEADS // CORES):
            att_in(m, g).wait_recv()

        def out_tile(t, carry):
            total = jnp.dot(att[m, 0], wo[:half, cols(t)], preferred_element_type=jnp.float32)
            total += jnp.dot(att[m, 1], wo[half:, cols(t)], preferred_element_type=jnp.float32)
            result = (hid[m, core, :, cols(t)].astype(jnp.float32) + total).astype(jnp.bfloat16)
            res[m, :, cols(t)] = result

            @pl.when(section < sections - 1)
            def _():
                hop(m, t).start()

            place_cols = pl.ds(pl.multiple_of(core * half + t * TILE, TILE), TILE)
            out_ref[m, :, place_cols] = res[m, own_rows, cols(t)]
            return carry

        lax.fori_loop(0, tiles, out_tile, 0)
        out_send(m).start()

    def turn(i, carry):
        @pl.when(i < micro)
        def _():
            front(i)

        @pl.when(i > 0)
        def _():
            back(i - 1)

        return carry

    lax.fori_loop(0, micro + 1, turn, 0)

    finish_weights(0)
    finish_weights(1)

    def finish(m, carry):
        @pl.when(first)
        def _():
            for h in range(2):
                x_send(m, h).wait_send()

        @pl.when(section > 0)
        def _():
            for t in range(tiles):
                relay(m, t).wait_send()

        @pl.when(section < sections - 1)
        def _():
            for t in range(tiles):
                hop(m, t).wait_send()

        for d in range(1, peers):
            kv_send(m, d).wait_send()
        for g in range(KV_HEADS // CORES):
            att_send(m, g).wait_send()
        out_send(m).wait_send()
        out_in(m).wait_recv()
        return carry

    lax.fori_loop(0, micro, finish, 0)


def doc_begin(positions, starts):
    at_or_below = starts[:, None, :] <= positions[:, :, None]
    return jnp.max(jnp.where(at_or_below, starts[:, None, :], 0), axis=2)


def body(x_in, norm_gain, w_qkv, w_out, cycle_size, token_pos, doc_starts):
    sections = lax.axis_size("pp")
    chips = lax.axis_size("cp") // CORES
    device = lax.axis_index("cp")
    micro, tok, width = x_in.shape
    rows = w_qkv.shape[1]
    total_tokens = token_pos.shape[1]
    half = width // 2
    query_cols = HEADS * HEAD_DIM
    key_cols = KV_HEADS * HEAD_DIM
    window = CYCLE_MAX * tok
    pair = CORES * tok

    block_start = device // CYCLE_MAX * window
    key_pos = lax.dynamic_slice_in_dim(token_pos, block_start, window, 1)
    key_begin = doc_begin(key_pos, doc_starts)
    key_code = key_pos // (cycle_size * tok)[:, None] * (total_tokens + 1) + key_begin
    inside = device % CYCLE_MAX // CORES * pair
    query_pos = lax.dynamic_slice_in_dim(key_pos, inside, pair, 1)
    query_begin = lax.dynamic_slice_in_dim(key_begin, inside, pair, 1)
    query_code = lax.dynamic_slice_in_dim(key_code, inside, pair, 1)
    frequency_index = jnp.arange(HEAD_DIM // 2, dtype=jnp.float32)
    inverse = jnp.power(jnp.float32(rope_base), -2.0 * frequency_index / HEAD_DIM)
    angles = (query_pos - query_begin).astype(jnp.float32)[:, :, None] * inverse
    cosine, sine = jnp.cos(angles), jnp.sin(angles)
    cos_full = jnp.concatenate([cosine, cosine], axis=-1)
    sin_full = jnp.concatenate([-sine, sine], axis=-1)

    def split(array):
        return jnp.stack(jnp.split(array, CORES, axis=1))

    wq_split = jnp.concatenate(
        [
            split(w_qkv[0][:, :query_cols]),
            split(w_qkv[0][:, query_cols : query_cols + key_cols]),
            split(w_qkv[0][:, query_cols + key_cols :]),
        ],
        axis=2,
    )
    wo_split = split(w_out[0])

    peers = CYCLE_MAX // CORES
    tiles = half // TILE
    bf = jnp.bfloat16
    dma = pltpu.SemaphoreType.DMA
    vmem = pl.BlockSpec(memory_space=pltpu.VMEM)
    outputs = pl.pallas_call(
        functools.partial(kernel, chips, sections),
        out_shape=jax.ShapeDtypeStruct((micro, tok, width), bf),
        in_specs=[vmem] * 10,
        out_specs=vmem,
        scratch_shapes=[
            pltpu.VMEM((width, wq_split.shape[2]), bf),
            pltpu.VMEM((query_cols, half), bf),
            pltpu.VMEM((micro, 2, pair, half), bf),
            pltpu.VMEM((pair, width), bf),
            pltpu.VMEM((micro, HEADS // CORES, pair, HEAD_DIM), bf),
            pltpu.VMEM((micro, peers, pair, 2 * key_cols // CORES), bf),
            pltpu.VMEM((micro, CORES, pair, query_cols // CORES), bf),
            pltpu.VMEM((micro, pair, half), bf),
            pltpu.VMEM((pair, window), jnp.float32),
            dma((2,)), dma((2,)),
            dma((2, chips)), dma((2, chips)), dma((2, chips)), dma((2, chips)),
            dma((micro, 2)), dma((micro, 2)),
            dma((2 + 2 * micro,)),
            dma((micro, tiles)), dma((micro, tiles)),
            dma((micro, tiles)), dma((micro, tiles)),
            dma((micro, peers - 1)), dma((micro, peers - 1)),
            dma((micro, KV_HEADS // CORES)), dma((micro, KV_HEADS // CORES)),
            dma((micro,)), dma((micro,)),
        ],
        compiler_params=pltpu.CompilerParams(has_side_effects=True, vmem_limit_bytes=60 * 1024 * 1024),
    )(
        x_in, norm_gain, wq_split, wo_split, cos_full, sin_full,
        query_pos[:, :, None], query_code[:, :, None], key_pos[:, None, :], key_code[:, None, :],
    )
    return outputs[None]


def solution(mesh):
    in_specs = (
        P(None, "cp", None),
        P("pp", None),
        P("pp", "cp", None),
        P("pp", "cp", None),
        P(),
        P(),
        P(),
    )
    out_specs = P("pp", None, "cp", None)
    return jax.shard_map(body, mesh=mesh, in_specs=in_specs, out_specs=out_specs, check_vma=False)
```
